8 devices in a mesh: dp: 1 (over z), ep: 8 (over y, x, core).
Axes of the slice: x: 2, y: 2, z: 1, core: 2. Of those that a mesh axis runs over, the one named last changes fastest.
Arguments:
- x_tokens: bfloat16 [12288, 2048], P(('dp', 'ep'))
- dy_tokens: bfloat16 [12288, 2048], P(('dp', 'ep'))
- expert_ids: int32 [12288, 6], P(('dp', 'ep'))
- gate_vals: float32 [12288, 6], P(('dp', 'ep'))
- slot_pos: int32 [12288, 6], P(('dp', 'ep'))
- w_gate: bfloat16 [16, 2048, 1408], P('ep')
- w_up: bfloat16 [16, 2048, 1408], P('ep')
- w_down: bfloat16 [16, 1408, 2048], P('ep')
- shared_gate: bfloat16 [2048, 2816], replicated
- shared_up: bfloat16 [2048, 2816], replicated
- shared_down: bfloat16 [2816, 2048], replicated
Outputs:
- output 1: bfloat16 [12288, 2048], P(('dp', 'ep'))
- output 2: float32 [16, 2048, 1408], P(('dp', 'ep'))
- output 3: float32 [16, 2048, 1408], P(('dp', 'ep'))
- output 4: float32 [16, 1408, 2048], P(('dp', 'ep'))
- output 5: float32 [8, 2048, 2816], P(('dp', 'ep'))
- output 6: float32 [8, 2048, 2816], P(('dp', 'ep'))
- output 7: float32 [8, 2816, 2048], P(('dp', 'ep'))
All inputs are finite; a program needn't handle non-finite values.
Results may differ from the reference program's by a relative error of at most 0.00174.
Values are sent between devices in bfloat16 or wider.
A program may use at most 1 GiB of HBM per device.

```python
import jax
import jax.numpy as jnp
from jax import lax

MODEL_DIM = 2048
EXPERT_FF = 1408
SHARED_FF = 2816
TOP_K = 6
TOK_DEV = 1536
GROUP_SIZE = 8
NUM_EXPERTS = 16
CAPACITY = 864


def draw_routing(route_key):
    bias_key, hot_key, noise_key = jax.random.split(route_key, 3)
    expert_range = jnp.arange(NUM_EXPERTS, dtype=jnp.int32)
    expert_bias = jax.random.randint(bias_key, (NUM_EXPERTS,), 0, 256)
    hot_expert = jax.random.randint(hot_key, (GROUP_SIZE,), 0, NUM_EXPERTS)
    noise = jax.random.randint(noise_key, (GROUP_SIZE, TOK_DEV, NUM_EXPERTS), 0, 1024)
    forced = (jnp.arange(TOK_DEV)[None, :, None] < CAPACITY) & (expert_range[None, None, :] == hot_expert[:, None, None])
    score = (noise + expert_bias[None, None, :] + 4096 * forced.astype(jnp.int32)) * NUM_EXPERTS + expert_range
    choices = lax.top_k(score, TOP_K)[1]

    def source_slots(source_choices):
        flat_choices = source_choices.reshape(-1)
        onehot = (flat_choices[:, None] == expert_range[None, :]).astype(jnp.int32)
        earlier = jnp.cumsum(onehot, axis=0) - onehot
        slot_rank = jnp.sum(earlier * onehot, axis=1)
        return jnp.where(slot_rank < CAPACITY, slot_rank, -1).reshape(TOK_DEV, TOP_K)

    positions = lax.map(source_slots, choices)
    return choices.reshape(-1, TOP_K).astype(jnp.int32), positions.reshape(-1, TOP_K).astype(jnp.int32)


def setup_inputs(seed: int = 0, part: int = 0) -> dict:
    part_key = jax.random.fold_in(jax.random.key(seed), part)
    key_x, key_dy, key_gate, key_route = jax.random.split(part_key, 4)
    weight_keys = jax.random.split(jax.random.key(seed + 1), 6)
    tokens = GROUP_SIZE * TOK_DEV
    x_tokens = jax.random.normal(key_x, (tokens, MODEL_DIM), jnp.float32).astype(jnp.bfloat16)
    dy_tokens = jax.random.normal(key_dy, (tokens, MODEL_DIM), jnp.float32).astype(jnp.bfloat16)
    gate_vals = jax.random.uniform(key_gate, (tokens, TOP_K), jnp.float32, 0.25, 1.0)
    expert_ids, slot_pos = draw_routing(key_route)
    in_scale = MODEL_DIM ** -0.5
    ff_scale = EXPERT_FF ** -0.5
    shared_scale = SHARED_FF ** -0.5
    w_gate = (jax.random.normal(weight_keys[0], (NUM_EXPERTS, MODEL_DIM, EXPERT_FF), jnp.float32) * in_scale).astype(jnp.bfloat16)
    w_up = (jax.random.normal(weight_keys[1], (NUM_EXPERTS, MODEL_DIM, EXPERT_FF), jnp.float32) * in_scale).astype(jnp.bfloat16)
    w_down = (jax.random.normal(weight_keys[2], (NUM_EXPERTS, EXPERT_FF, MODEL_DIM), jnp.float32) * ff_scale).astype(jnp.bfloat16)
    shared_gate = (jax.random.normal(weight_keys[3], (MODEL_DIM, SHARED_FF), jnp.float32) * in_scale).astype(jnp.bfloat16)
    shared_up = (jax.random.normal(weight_keys[4], (MODEL_DIM, SHARED_FF), jnp.float32) * in_scale).astype(jnp.bfloat16)
    shared_down = (jax.random.normal(weight_keys[5], (SHARED_FF, MODEL_DIM), jnp.float32) * shared_scale).astype(jnp.bfloat16)
    return {'x_tokens': x_tokens, 'dy_tokens': dy_tokens, 'expert_ids': expert_ids, 'gate_vals': gate_vals, 'slot_pos': slot_pos, 'w_gate': w_gate, 'w_up': w_up, 'w_down': w_down, 'shared_gate': shared_gate, 'shared_up': shared_up, 'shared_down': shared_down}


def expert_grads(x_rows, dz_rows, gate_w, up_w, down_w):
    act_gate = jnp.dot(x_rows, gate_w, preferred_element_type=jnp.float32).astype(jnp.bfloat16)
    act_up = jnp.dot(x_rows, up_w, preferred_element_type=jnp.float32).astype(jnp.bfloat16)
    gate_f32 = act_gate.astype(jnp.float32)
    up_f32 = act_up.astype(jnp.float32)
    sigma = jax.nn.sigmoid(gate_f32)
    silu_gate = gate_f32 * sigma
    hidden = (silu_gate * up_f32).astype(jnp.bfloat16)
    grad_hidden = jnp.dot(dz_rows, down_w.T, preferred_element_type=jnp.float32)
    grad_gate = (grad_hidden * up_f32 * sigma * (1.0 + gate_f32 * (1.0 - sigma))).astype(jnp.bfloat16)
    grad_up = (grad_hidden * silu_gate).astype(jnp.bfloat16)
    grad_down_w = jnp.dot(hidden.T, dz_rows, preferred_element_type=jnp.float32)
    grad_gate_w = jnp.dot(x_rows.T, grad_gate, preferred_element_type=jnp.float32)
    grad_up_w = jnp.dot(x_rows.T, grad_up, preferred_element_type=jnp.float32)
    grad_rows = jnp.dot(grad_gate, gate_w.T, preferred_element_type=jnp.float32) + jnp.dot(grad_up, up_w.T, preferred_element_type=jnp.float32)
    return grad_rows, grad_gate_w, grad_up_w, grad_down_w


def reference(x_tokens, dy_tokens, expert_ids, gate_vals, slot_pos, w_gate, w_up, w_down, shared_gate, shared_up, shared_down):
    tokens = GROUP_SIZE * TOK_DEV
    slot_rows = GROUP_SIZE * CAPACITY
    total_rows = NUM_EXPERTS * slot_rows
    source = jnp.arange(tokens, dtype=jnp.int32)[:, None] // TOK_DEV
    target = jnp.where(slot_pos >= 0, expert_ids * slot_rows + source * CAPACITY + slot_pos, total_rows).reshape(-1)
    token_index = jnp.broadcast_to(jnp.arange(tokens, dtype=jnp.int32)[:, None], (tokens, TOP_K)).reshape(-1)
    row_token = jnp.full((total_rows + 1,), tokens, jnp.int32).at[target].set(token_index)[:total_rows].reshape(NUM_EXPERTS, slot_rows)
    row_gate = jnp.zeros((total_rows + 1,), jnp.float32).at[target].set(gate_vals.reshape(-1))[:total_rows].reshape(NUM_EXPERTS, slot_rows)

    def expert_step(routed_sum, expert_in):
        token_rows, gate_rows, gate_w, up_w, down_w = expert_in
        x_rows = jnp.take(x_tokens, token_rows, axis=0, mode='fill', fill_value=0)
        dy_rows = jnp.take(dy_tokens, token_rows, axis=0, mode='fill', fill_value=0)
        dz_rows = (dy_rows.astype(jnp.float32) * gate_rows[:, None]).astype(jnp.bfloat16)
        grad_rows, grad_gate_w, grad_up_w, grad_down_w = expert_grads(x_rows, dz_rows, gate_w, up_w, down_w)
        returned = grad_rows.astype(jnp.bfloat16).astype(jnp.float32)
        routed_sum = routed_sum.at[token_rows].add(returned, mode='drop')
        return routed_sum, (grad_gate_w, grad_up_w, grad_down_w)

    routed_sum, expert_w_grads = lax.scan(expert_step, jnp.zeros((tokens, MODEL_DIM), jnp.float32), (row_token, row_gate, w_gate, w_up, w_down))
    grad_w_gate, grad_w_up, grad_w_down = expert_w_grads

    def shared_step(source_in):
        x_rows, dy_rows = source_in
        return expert_grads(x_rows, dy_rows, shared_gate, shared_up, shared_down)

    shared_dx, grad_shared_gate, grad_shared_up, grad_shared_down = lax.map(shared_step, (x_tokens.reshape(GROUP_SIZE, TOK_DEV, MODEL_DIM), dy_tokens.reshape(GROUP_SIZE, TOK_DEV, MODEL_DIM)))
    grad_x = (routed_sum + shared_dx.reshape(tokens, MODEL_DIM)).astype(jnp.bfloat16)
    return (grad_x, grad_w_gate, grad_w_up, grad_w_down, grad_shared_gate, grad_shared_up, grad_shared_down)
```

```python
import functools

import jax
import jax.numpy as jnp
from jax import lax
from jax.experimental import pallas as pl
from jax.experimental.pallas import tpu as pltpu
from jax.sharding import PartitionSpec as P

BF16, F32, I32 = jnp.bfloat16, jnp.float32, jnp.int32
TB = 256
TM = 512
CHUNKS = 2
VMEM = 64 * 1024 * 1024 - 128 * 1024


def dot(a, b):
    return lax.dot_general(a, b, (((1,), (0,)), ((), ())), preferred_element_type=F32)


def dot_t(a, b):
    return lax.dot_general(a, b, (((1,), (1,)), ((), ())), preferred_element_type=F32)


def params(ndim):
    return pltpu.CompilerParams(dimension_semantics=("arbitrary",) * ndim, vmem_limit_bytes=VMEM)


def swiglu_parts(act_gate, act_up, grad_hidden):
    gate_f32 = act_gate.astype(F32)
    up_f32 = act_up.astype(F32)
    sigma = jax.nn.sigmoid(gate_f32)
    silu_gate = gate_f32 * sigma
    hidden = (silu_gate * up_f32).astype(BF16)
    grad_gate = (grad_hidden * up_f32 * sigma * (1.0 + gate_f32 * (1.0 - sigma))).astype(BF16)
    grad_up = (grad_hidden * silu_gate).astype(BF16)
    return hidden, grad_gate, grad_up


def pack_kernel(tile_ref, x_ref, dy_ref, pos_ref, gate_ref, *refs):
    xo_ref, zo_ref = refs[-2:]
    e, b, k = pl.program_id(0), pl.program_id(1), pl.program_id(2)
    blocks = pl.num_programs(1) - 1
    step = 2 * b + k
    tile = tile_ref[e, step]
    before = tile_ref[e, jnp.maximum(step - 1, 0)]
    fresh = (step == 0) | (tile != before)

    @pl.when(fresh)
    def _():
        xo_ref[...] = jnp.zeros_like(xo_ref)
        zo_ref[...] = jnp.zeros_like(zo_ref)

    @pl.when((b < blocks) & ((k == 0) | fresh))
    def _():
        local = pos_ref[0, 0] - tile * TB
        hit = lax.broadcasted_iota(I32, (TB, TB), 0) == local
        row_gate = jnp.sum(jnp.where(hit, gate_ref[0, 0], 0.0), axis=1, keepdims=True)
        pick = hit.astype(F32).astype(BF16)
        xo_ref[0] += dot(pick, x_ref[...]).astype(BF16)
        zo_ref[0] += (dot(pick, dy_ref[...]) * row_gate).astype(BF16)


def pack_rows(tiles, x, dy, pos, gate, after):
    experts, blocks = pos.shape[:2]
    rows, dim = x.shape
    tok = lambda e, b, k, t: (jnp.minimum(b, blocks - 1), 0)
    row = lambda e, b, k, t: (e, jnp.minimum(b, blocks - 1), 0, 0)
    out = lambda e, b, k, t: (e, t[e, 2 * b + k], 0)
    return pl.pallas_call(
        pack_kernel,
        grid_spec=pltpu.PrefetchScalarGridSpec(
            num_scalar_prefetch=1, grid=(experts, blocks + 1, 2),
            in_specs=[pl.BlockSpec((TB, dim), tok), pl.BlockSpec((TB, dim), tok),
                      pl.BlockSpec((1, 1, 1, TB), row), pl.BlockSpec((1, 1, 1, TB), row)] + [pl.BlockSpec(memory_space=pl.ANY)] * len(after),
            out_specs=[pl.BlockSpec((1, TB, dim), out), pl.BlockSpec((1, TB, dim), out)]),
        out_shape=[jax.ShapeDtypeStruct((experts, rows, dim), BF16)] * 2,
        compiler_params=params(3),
        cost_estimate=pl.CostEstimate(flops=30_000_000_000, bytes_accessed=200_000_000, transcendentals=0),
        name="pack_rows",
    )(tiles, x, dy, pos, gate, *after)


def ffn_kernel(n_ref, x_ref, z_ref, w1_ref, w3_ref, w2_ref, h_ref, d_ref, r_ref):
    ff = w1_ref.shape[2]
    dim = w1_ref.shape[1]

    @pl.when(pl.program_id(1) < n_ref[pl.program_id(0)])
    def _():
        def columns(lo, size, act_gate, act_up):
            grad_hidden = dot_t(z_ref[0], w2_ref[0, lo:lo + size, :])
            hidden, grad_gate, grad_up = swiglu_parts(act_gate.astype(BF16), act_up.astype(BF16), grad_hidden)
            h_ref[0, :, lo:lo + size] = hidden
            d_ref[0, :, lo:lo + size] = grad_gate
            d_ref[0, :, ff + lo:ff + lo + size] = grad_up

        full = ff // 256 * 256
        for lo in range(0, full, 256):
            columns(lo, 256, dot(x_ref[0], w1_ref[0, :, lo:lo + 256]), dot(x_ref[0], w3_ref[0, :, lo:lo + 256]))
        if full < ff:
            both = dot(x_ref[0], jnp.concatenate([w1_ref[0, :, full:], w3_ref[0, :, full:]], axis=1))
            columns(full, ff - full, both[:, :ff - full], both[:, ff - full:])
        for lo in range(0, dim, 256):
            w = jnp.concatenate([w1_ref[0, lo:lo + 256, :], w3_ref[0, lo:lo + 256, :]], axis=1)
            r_ref[0, :, lo:lo + 256] = dot_t(d_ref[0], w).astype(r_ref.dtype)


def ffn_tiles(active, x, z, w1, w3, w2, out_dtype, tm, name):
    experts, rows, dim = x.shape
    ff = w1.shape[2]
    tile = lambda e, m, n: (e, jnp.minimum(m, n[e] - 1), 0)
    whole = lambda e, m, n: (e, 0, 0)
    return pl.pallas_call(
        ffn_kernel,
        grid_spec=pltpu.PrefetchScalarGridSpec(
            num_scalar_prefetch=1, grid=(experts, rows // tm),
            in_specs=[pl.BlockSpec((1, tm, dim), tile), pl.BlockSpec((1, tm, dim), tile),
                      pl.BlockSpec((1, dim, ff), whole, pipeline_mode=pl.Buffered(1)),
                      pl.BlockSpec((1, dim, ff), whole, pipeline_mode=pl.Buffered(1)),
                      pl.BlockSpec((1, ff, dim), whole, pipeline_mode=pl.Buffered(1))],
            out_specs=[pl.BlockSpec((1, tm, ff), tile), pl.BlockSpec((1, tm, 2 * ff), tile),
                       pl.BlockSpec((1, tm, dim), tile)]),
        out_shape=[jax.ShapeDtypeStruct((experts, rows, ff), BF16),
                   jax.ShapeDtypeStruct((experts, rows, 2 * ff), BF16),
                   jax.ShapeDtypeStruct((experts, rows, dim), out_dtype)],
        compiler_params=params(2),
        cost_estimate=pl.CostEstimate(flops=5 * rows * dim * ff, bytes_accessed=150_000_000, transcendentals=0),
        name=name,
    )(active, x, z, w1, w3, w2)


def tile_maps(chunks):
    def maker(c, cols):
        def index(e, d, j, n):
            first = sum((n[q, e] for q in range(c)), 0)
            return (e, jnp.clip(j - first, 0, n[c, e] - 1), d if cols else 0)
        return index
    return [maker(c, False) for c in range(chunks)], [maker(c, True) for c in range(chunks)]


def for_chunk(n_ref, chunks, body):
    e, j = pl.program_id(0), pl.program_id(2)
    first = 0
    for c in range(chunks):
        last = first + n_ref[c, e]
        pl.when((j >= first) & (j < last))(functools.partial(body, c))
        first = last


def up_grad_kernel(chunks, n_ref, *refs):
    xs, ds = refs[:chunks], refs[chunks:2 * chunks]
    g1_ref, g3_ref = refs[2 * chunks:]
    ff = g1_ref.shape[2]

    @pl.when(pl.program_id(2) == 0)
    def _():
        g1_ref[...] = jnp.zeros_like(g1_ref)
        g3_ref[...] = jnp.zeros_like(g3_ref)

    def body(c):
        x_t = xs[c][0].T
        for lo in range(0, 2 * ff, 256):
            part = dot(x_t, ds[c][0, :, lo:lo + 256])
            if lo + 256 <= ff:
                g1_ref[0, :, lo:lo + 256] += part
            elif lo >= ff:
                g3_ref[0, :, lo - ff:lo - ff + 256] += part
            else:
                g1_ref[0, :, lo:] += part[:, :ff - lo]
                g3_ref[0, :, :lo + 256 - ff] += part[:, ff - lo:]

    for_chunk(n_ref, chunks, body)


def up_grads(active, xs, ds, split):
    chunks = len(xs)
    experts, rows, dim = xs[0].shape
    ff = ds[0].shape[2] // 2
    whole, cols = tile_maps(chunks)
    out = lambda e, d, j, n: (e, d, 0)
    return pl.pallas_call(
        functools.partial(up_grad_kernel, chunks),
        grid_spec=pltpu.PrefetchScalarGridSpec(
            num_scalar_prefetch=1, grid=(experts, split, chunks * (rows // TM)),
            in_specs=[pl.BlockSpec((1, TM, dim // split), m) for m in cols] + [pl.BlockSpec((1, TM, 2 * ff), m) for m in whole],
            out_specs=[pl.BlockSpec((1, dim // split, ff), out)] * 2),
        out_shape=[jax.ShapeDtypeStruct((experts, dim, ff), F32)] * 2,
        compiler_params=params(3),
        cost_estimate=pl.CostEstimate(flops=120_000_000_000, bytes_accessed=250_000_000, transcendentals=0),
        name="up_grads",
    )(active, *xs, *ds)


def down_grad_kernel(chunks, n_ref, *refs):
    hs, zs = refs[:chunks], refs[chunks:2 * chunks]
    g_ref = refs[2 * chunks]

    @pl.when(pl.program_id(2) == 0)
    def _():
        g_ref[...] = jnp.zeros_like(g_ref)

    def body(c):
        h_t = hs[c][0].T
        for lo in range(0, g_ref.shape[2], 256):
            g_ref[0, :, lo:lo + 256] += dot(h_t, zs[c][0, :, lo:lo + 256])

    for_chunk(n_ref, chunks, body)


def down_grads(active, hs, zs, split):
    chunks = len(hs)
    experts, rows, ff = hs[0].shape
    dim = zs[0].shape[2]
    whole, cols = tile_maps(chunks)
    return pl.pallas_call(
        functools.partial(down_grad_kernel, chunks),
        grid_spec=pltpu.PrefetchScalarGridSpec(
            num_scalar_prefetch=1, grid=(experts, split, chunks * (rows // TM)),
            in_specs=[pl.BlockSpec((1, TM, ff), m) for m in whole] + [pl.BlockSpec((1, TM, dim // split), m) for m in cols],
            out_specs=[pl.BlockSpec((1, ff, dim // split), lambda e, d, j, n: (e, 0, d))]),
        out_shape=[jax.ShapeDtypeStruct((experts, ff, dim), F32)],
        compiler_params=params(3),
        cost_estimate=pl.CostEstimate(flops=60_000_000_000, bytes_accessed=150_000_000, transcendentals=0),
        name="down_grads",
    )(active, *hs, *zs)[0]


def token_sum_kernel(experts, lo_ref, hi_ref, pos_ref, *refs):
    b = pl.program_id(0)
    out_ref = refs[-1]
    picks, rows = [], []
    for e in range(experts):
        for near, tile_ref in enumerate((lo_ref, hi_ref)):
            tile = tile_ref[e, b]
            local = jnp.where(tile < 0, -1, pos_ref[e, 0] - tile * TB)
            picks.append((lax.broadcasted_iota(I32, (TB, TB), 0) == local).astype(F32).T.astype(BF16))
            rows.append(refs[2 * e + near][0])
    out_ref[...] = dot(jnp.concatenate(picks, axis=1), jnp.concatenate(rows, axis=0))


def token_sums(lo, hi, pos, r):
    experts, blocks = pos.shape[:2]
    dim = r.shape[2]
    specs = []
    for e in range(experts):
        specs.append(pl.BlockSpec((1, TB, dim), lambda b, l, h, e=e: (e, jnp.maximum(l[e, b], 0), 0)))
        specs.append(pl.BlockSpec((1, TB, dim), lambda b, l, h, e=e: (e, jnp.maximum(h[e, b], 0), 0)))
    return pl.pallas_call(
        functools.partial(token_sum_kernel, experts),
        grid_spec=pltpu.PrefetchScalarGridSpec(
            num_scalar_prefetch=2, grid=(blocks,),
            in_specs=[pl.BlockSpec((experts, 1, 1, TB), lambda b, l, h: (0, b, 0, 0))] + specs,
            out_specs=[pl.BlockSpec((TB, dim), lambda b, l, h: (b, 0))]),
        out_shape=[jax.ShapeDtypeStruct((blocks * TB, dim), F32)],
        compiler_params=params(1),
        cost_estimate=pl.CostEstimate(flops=20_000_000_000, bytes_accessed=100_000_000, transcendentals=0),
        name="token_sums",
    )(lo, hi, pos, *([r] * (2 * experts)))[0]


def shared_backward(x, dy, gate_w, up_w, down_w):
    x, dy = x[None], dy[None]
    tm = x.shape[1] // 4
    all_tiles = lambda size: jnp.full((1,), x.shape[1] // size, I32)
    hidden, grads, back = ffn_tiles(all_tiles(tm), x, dy, gate_w[None], up_w[None], down_w[None], F32, tm, "shared_ffn")
    grad_gate, grad_up = up_grads(all_tiles(TM)[None], [x], [grads], 4)
    grad_down = down_grads(all_tiles(TM)[None], [hidden], [dy], 2)
    return back[0], grad_gate, grad_up, grad_down


def chunk_tables(codes, gates, experts):
    top_k, tokens = codes.shape
    blocks = tokens // TB
    ids = lax.axis_index('ep') * experts + jnp.arange(experts, dtype=I32)
    match = codes[None] == ids[:, None, None].astype(F32)
    hit = jnp.any(match, axis=1).reshape(experts, blocks, TB)
    gate = jnp.sum(jnp.where(match, gates[None], 0.0), axis=1).reshape(experts, blocks, 1, TB)
    tri = (jnp.arange(TB)[:, None] < jnp.arange(TB)[None, :]).astype(BF16)
    rank = jnp.dot(hit.reshape(-1, TB).astype(BF16), tri, preferred_element_type=F32).astype(I32).reshape(experts, blocks, TB)
    count = jnp.sum(hit.astype(I32), axis=2)
    below = jnp.arange(blocks)[:, None] < jnp.arange(blocks)[None, :]
    start = jnp.sum(jnp.where(below[None], count[:, :, None], 0), axis=1)
    total = start[:, -1] + count[:, -1]
    pos = jnp.where(hit, start[:, :, None] + rank, -(1 << 20)).reshape(experts, blocks, 1, TB)
    active = jnp.maximum((total + TM - 1) // TM, 1)
    small_last = jnp.maximum((total + TB - 1) // TB, 1)[:, None] - 1
    lo = jnp.minimum(start // TB, small_last)
    hi = jnp.clip((start + count - 1) // TB, lo, small_last)
    visits = jnp.stack([lo, hi], axis=2).reshape(experts, 2 * blocks)
    tail = (active * (TM // TB) - 1)[:, None]
    visits = jnp.concatenate([visits, tail, tail], axis=1)
    some = count > 0
    return visits, active, jnp.where(some, lo, -1), jnp.where(some & (hi > lo), hi, -1), pos, gate


def solution(mesh):
    group = mesh.shape['ep']
    token_spec = P(('dp', 'ep'), None)
    expert_spec = P('ep', None, None)
    whole_spec = P(None, None)
    grad_spec = P(('dp', 'ep'), None, None)

    def local_backward(x_tokens, dy_tokens, expert_ids, gate_vals, slot_pos, w_gate, w_up, w_down, shared_gate, shared_up, shared_down):
        tok_count, top_k = expert_ids.shape
        local_experts = w_gate.shape[0]
        part = tok_count // CHUNKS
        codes = jnp.where(slot_pos >= 0, expert_ids, -1).astype(F32).T
        plan = lax.all_gather(jnp.concatenate([codes, gate_vals.T], axis=0), 'ep', axis=0)
        gathered = []
        for c in range(CHUNKS):
            rows = slice(c * part, (c + 1) * part)
            gathered.append((lax.all_gather(x_tokens[rows], 'ep', axis=0, tiled=True), lax.all_gather(dy_tokens[rows], 'ep', axis=0, tiled=True)))
        shared = shared_backward(x_tokens, dy_tokens, shared_gate, shared_up, shared_down)
        shared_dx, grad_shared_gate, grad_shared_up, grad_shared_down = shared
        packed = []
        for c in range(CHUNKS):
            mine = plan[:, :, c * part:(c + 1) * part].transpose(1, 0, 2).reshape(2 * top_k, group * part)
            visits, active, lo, hi, pos, gate = chunk_tables(mine[:top_k], mine[top_k:], local_experts)
            x_rows, z_rows = pack_rows(visits, *gathered[c], pos, gate, shared[1:] if c == 0 else ())
            hidden, grads, back = ffn_tiles(active, x_rows, z_rows, w_gate, w_up, w_down, BF16, TM, "ffn_tiles")
            summed = lax.psum_scatter(token_sums(lo, hi, pos, back), 'ep', scatter_dimension=0, tiled=True)
            packed.append((active, x_rows, z_rows, hidden, grads, summed))
        active, x_rows, z_rows, hidden, grads, summed = zip(*packed)
        active = jnp.stack(active)
        grad_w_gate, grad_w_up = up_grads(active, x_rows, grads, 2)
        grad_w_down = down_grads(active, hidden, z_rows, 1)
        grad_x = (jnp.concatenate(summed, axis=0) + shared_dx).astype(BF16)
        return grad_x, grad_w_gate, grad_w_up, grad_w_down, grad_shared_gate, grad_shared_up, grad_shared_down

    return jax.shard_map(local_backward, mesh=mesh, in_specs=(token_spec, token_spec, token_spec, token_spec, token_spec, expert_spec, expert_spec, expert_spec, whole_spec, whole_spec, whole_spec), out_specs=(token_spec, grad_spec, grad_spec, grad_spec, grad_spec, grad_spec, grad_spec), check_vma=False)
```

```python
import functools

import jax
import jax.numpy as jnp
from jax import lax
from jax.experimental import pallas as pl
from jax.experimental.pallas import tpu as pltpu
from jax.sharding import PartitionSpec as P

BF16, F32, I32 = jnp.bfloat16, jnp.float32, jnp.int32
TB = 256
TM = 512
WINDOW = 768
CHUNKS = 3
VMEM = 64 * 1024 * 1024 - 128 * 1024


def dot(a, b):
    return lax.dot_general(a, b, (((1,), (0,)), ((), ())), preferred_element_type=F32)


def dot_t(a, b):
    return lax.dot_general(a, b, (((1,), (1,)), ((), ())), preferred_element_type=F32)


def params(ndim):
    return pltpu.CompilerParams(dimension_semantics=("arbitrary",) * ndim, vmem_limit_bytes=VMEM)


def swiglu_parts(act_gate, act_up, grad_hidden):
    gate_f32 = act_gate.astype(F32)
    up_f32 = act_up.astype(F32)
    sigma = jax.nn.sigmoid(gate_f32)
    silu_gate = gate_f32 * sigma
    hidden = (silu_gate * up_f32).astype(BF16)
    grad_gate = (grad_hidden * up_f32 * sigma * (1.0 + gate_f32 * (1.0 - sigma))).astype(BF16)
    grad_up = (grad_hidden * silu_gate).astype(BF16)
    return hidden, grad_gate, grad_up


def pack_kernel(first_ref, window_ref, n_ref, x_ref, dy_ref, pos_ref, gate_ref, *refs):
    xo_ref, zo_ref = refs[-2:]
    e, m = pl.program_id(0), pl.program_id(1)
    tokens = x_ref.shape[0]

    def window(w):
        wanted = first_ref[e, m] + w * WINDOW
        begin = pl.multiple_of(jnp.minimum(wanted, tokens - WINDOW), 128)
        at = pl.ds(begin, WINDOW)
        token = begin + lax.broadcasted_iota(I32, (1, WINDOW), 1)
        local = jnp.where(token >= wanted, pos_ref[0, :, at] - m * TB, -1)
        hit = lax.broadcasted_iota(I32, (TB, WINDOW), 0) == local
        row_gate = jnp.sum(jnp.where(hit, gate_ref[0, :, at], 0.0), axis=1, keepdims=True)
        pick = hit.astype(F32).astype(BF16)
        return dot(pick, x_ref[at, :]).astype(BF16), (dot(pick, dy_ref[at, :]) * row_gate).astype(BF16)

    @pl.when(m < n_ref[e])
    def _():
        xo_ref[0], zo_ref[0] = window(0)

    def more(w, carry):
        x_rows, z_rows = window(w)
        xo_ref[0] += x_rows
        zo_ref[0] += z_rows
        return carry

    lax.fori_loop(1, jnp.where(m < n_ref[e], window_ref[e, m], 1), more, 0)


def pack_rows(first, windows, units, x, dy, pos, gate, chunk, held, after):
    experts = pos.shape[0]
    rows, dim = x.shape
    tok = pl.BlockSpec((rows, dim), lambda e, m, f, w, n: (0, 0), pipeline_mode=pl.Buffered(1))
    row = pl.BlockSpec((1, 1, rows), lambda e, m, f, w, n: (e, 0, 0))
    out = pl.BlockSpec((1, TB, dim), lambda e, m, f, w, n: (e, chunk * (rows // TB) + jnp.minimum(m, n[e] - 1), 0))
    return pl.pallas_call(
        pack_kernel,
        grid_spec=pltpu.PrefetchScalarGridSpec(
            num_scalar_prefetch=3, grid=(experts, rows // TB),
            in_specs=[tok, tok, row, row] + [pl.BlockSpec(memory_space=pl.ANY)] * (len(held) + len(after)),
            out_specs=[out, out]),
        out_shape=[jax.ShapeDtypeStruct((experts, CHUNKS * rows, dim), BF16)] * 2,
        input_output_aliases={7 + i: i for i in range(len(held))},
        compiler_params=params(2),
        cost_estimate=pl.CostEstimate(flops=30_000_000_000, bytes_accessed=200_000_000, transcendentals=0),
        name="pack_rows",
    )(first, windows, units, x, dy, pos, gate, *held, *after)


def ffn_kernel(sizes, n_ref, x_ref, z_ref, w1_ref, w3_ref, w2_ref, *refs):
    h_ref, d_ref, r_ref = refs[-3:]
    ff = w1_ref.shape[2]
    dim = w1_ref.shape[1]
    left = n_ref[pl.program_id(0)] - len(sizes) * pl.program_id(1)

    def tile(rows):
        def columns(lo, size, act_gate, act_up):
            grad_hidden = dot_t(z_ref[0, :rows], w2_ref[0, lo:lo + size, :])
            hidden, grad_gate, grad_up = swiglu_parts(act_gate.astype(BF16), act_up.astype(BF16), grad_hidden)
            h_ref[0, :rows, lo:lo + size] = hidden
            d_ref[0, :rows, lo:lo + size] = grad_gate
            d_ref[0, :rows, ff + lo:ff + lo + size] = grad_up

        full = ff // 256 * 256
        for lo in range(0, full, 256):
            columns(lo, 256, dot(x_ref[0, :rows], w1_ref[0, :, lo:lo + 256]), dot(x_ref[0, :rows], w3_ref[0, :, lo:lo + 256]))
        if full < ff:
            both = dot(x_ref[0, :rows], jnp.concatenate([w1_ref[0, :, full:], w3_ref[0, :, full:]], axis=1))
            columns(full, ff - full, both[:, :ff - full], both[:, ff - full:])
        for lo in range(0, dim, 256):
            w = jnp.concatenate([w1_ref[0, lo:lo + 256, :], w3_ref[0, lo:lo + 256, :]], axis=1)
            r_ref[0, :rows, lo:lo + 256] = dot_t(d_ref[0, :rows], w).astype(r_ref.dtype)

    for i, rows in enumerate(sizes):
        pl.when((left == i + 1) if i + 1 < len(sizes) else (left > i))(functools.partial(tile, rows))


def ffn_tiles(units, x, z, w1, w3, w2, out_dtype, sizes, chunks, chunk, held, name):
    experts, dim, ff = w1.shape
    rows = x.shape[1] // chunks
    tm, per = sizes[-1], len(sizes)
    inner = lambda e, m, n: jnp.minimum(m, (n[e] + per - 1) // per - 1)
    tile = lambda e, m, n: (e, chunk * (rows // tm) + inner(e, m, n), 0)
    whole = lambda e, m, n: (e, 0, 0)
    return pl.pallas_call(
        functools.partial(ffn_kernel, sizes),
        grid_spec=pltpu.PrefetchScalarGridSpec(
            num_scalar_prefetch=1, grid=(experts, rows // tm),
            in_specs=[pl.BlockSpec((1, tm, dim), tile), pl.BlockSpec((1, tm, dim), tile),
                      pl.BlockSpec((1, dim, ff), whole, pipeline_mode=pl.Buffered(1)),
                      pl.BlockSpec((1, dim, ff), whole, pipeline_mode=pl.Buffered(1)),
                      pl.BlockSpec((1, ff, dim), whole, pipeline_mode=pl.Buffered(1))] + [pl.BlockSpec(memory_space=pl.ANY)] * len(held),
            out_specs=[pl.BlockSpec((1, tm, ff), tile), pl.BlockSpec((1, tm, 2 * ff), tile),
                       pl.BlockSpec((1, tm, dim), lambda e, m, n: (e, inner(e, m, n), 0))]),
        out_shape=[jax.ShapeDtypeStruct((experts, chunks * rows, ff), BF16),
                   jax.ShapeDtypeStruct((experts, chunks * rows, 2 * ff), BF16),
                   jax.ShapeDtypeStruct((experts, rows, dim), out_dtype)],
        input_output_aliases={6 + i: i for i in range(len(held))},
        compiler_params=params(2),
        cost_estimate=pl.CostEstimate(flops=5 * experts * rows * dim * ff, bytes_accessed=150_000_000, transcendentals=0),
        name=name,
    )(units, x, z, w1, w3, w2, *held)


def for_tile(sizes, left_ref, body):
    left = left_ref[pl.program_id(0), pl.program_id(2)]
    for i, rows in enumerate(sizes):
        pl.when((left == i + 1) if i + 1 < len(sizes) else (left > i))(functools.partial(body, rows))


def up_grad_kernel(sizes, tile_ref, left_ref, x_ref, d_ref, g1_ref, g3_ref):
    ff = g1_ref.shape[2]

    @pl.when(pl.program_id(2) == 0)
    def _():
        g1_ref[...] = jnp.zeros_like(g1_ref)
        g3_ref[...] = jnp.zeros_like(g3_ref)

    def body(rows):
        x_t = x_ref[0, :rows].T
        for lo in range(0, 2 * ff, 256):
            part = dot(x_t, d_ref[0, :rows, lo:lo + 256])
            if lo + 256 <= ff:
                g1_ref[0, :, lo:lo + 256] += part
            elif lo >= ff:
                g3_ref[0, :, lo - ff:lo - ff + 256] += part
            else:
                g1_ref[0, :, lo:] += part[:, :ff - lo]
                g3_ref[0, :, :lo + 256 - ff] += part[:, ff - lo:]

    for_tile(sizes, left_ref, body)


def up_grads(tiles, left, x, d, split, sizes):
    experts, _, dim = x.shape
    ff = d.shape[2] // 2
    out = lambda e, s, j, t, n: (e, s, 0)
    return pl.pallas_call(
        functools.partial(up_grad_kernel, sizes),
        grid_spec=pltpu.PrefetchScalarGridSpec(
            num_scalar_prefetch=2, grid=(experts, split, tiles.shape[1]),
            in_specs=[pl.BlockSpec((1, TM, dim // split), lambda e, s, j, t, n: (e, t[e, j], s)),
                      pl.BlockSpec((1, TM, 2 * ff), lambda e, s, j, t, n: (e, t[e, j], 0))],
            out_specs=[pl.BlockSpec((1, dim // split, ff), out)] * 2),
        out_shape=[jax.ShapeDtypeStruct((experts, dim, ff), F32)] * 2,
        compiler_params=params(3),
        cost_estimate=pl.CostEstimate(flops=120_000_000_000, bytes_accessed=250_000_000, transcendentals=0),
        name="up_grads",
    )(tiles, left, x, d)


def down_grad_kernel(sizes, tile_ref, left_ref, h_ref, z_ref, g_ref):
    @pl.when(pl.program_id(2) == 0)
    def _():
        g_ref[...] = jnp.zeros_like(g_ref)

    def body(rows):
        h_t = h_ref[0, :rows].T
        for lo in range(0, g_ref.shape[2], 256):
            g_ref[0, :, lo:lo + 256] += dot(h_t, z_ref[0, :rows, lo:lo + 256])

    for_tile(sizes, left_ref, body)


def down_grads(tiles, left, h, z, split, sizes):
    experts, _, ff = h.shape
    dim = z.shape[2]
    return pl.pallas_call(
        functools.partial(down_grad_kernel, sizes),
        grid_spec=pltpu.PrefetchScalarGridSpec(
            num_scalar_prefetch=2, grid=(experts, split, tiles.shape[1]),
            in_specs=[pl.BlockSpec((1, TM, ff), lambda e, s, j, t, n: (e, t[e, j], 0)),
                      pl.BlockSpec((1, TM, dim // split), lambda e, s, j, t, n: (e, t[e, j], s))],
            out_specs=[pl.BlockSpec((1, ff, dim // split), lambda e, s, j, t, n: (e, 0, s))]),
        out_shape=[jax.ShapeDtypeStruct((experts, ff, dim), F32)],
        compiler_params=params(3),
        cost_estimate=pl.CostEstimate(flops=60_000_000_000, bytes_accessed=150_000_000, transcendentals=0),
        name="down_grads",
    )(tiles, left, h, z)[0]


def gradient_tiles(units, chunk_tiles, steps):
    per = TM // TB
    tiles = (units + per - 1) // per
    ends = jnp.cumsum(tiles, axis=0)
    j = jnp.arange(steps, dtype=I32)
    j_in = jnp.minimum(j[None, :], ends[-1][:, None] - 1)
    chunk = jnp.sum((j_in[None] >= ends[:, :, None]).astype(I32), axis=0)
    begin = jnp.sum(jnp.where(jnp.arange(len(units))[:, None, None] < chunk[None], tiles[:, :, None], 0), axis=0)
    count = jnp.sum(jnp.where(jnp.arange(len(units))[:, None, None] == chunk[None], units[:, :, None], 0), axis=0)
    inner = j_in - begin
    left = jnp.where(j[None, :] < ends[-1][:, None], count - per * inner, 0)
    return (chunk * chunk_tiles + inner).astype(I32), left.astype(I32)


def token_sum_kernel(experts, lo_ref, hi_ref, pos_ref, *refs):
    b = pl.program_id(0)
    out_ref = refs[-1]
    picks, rows = [], []
    for e in range(experts):
        for near in range(2):
            tile = hi_ref[e, b] if near else lo_ref[e, b]
            local = pos_ref[e, 0] - tile * TB
            if near:
                local = jnp.where(tile == lo_ref[e, b], -1, local)
            picks.append((lax.broadcasted_iota(I32, (TB, TB), 0) == local).astype(F32).T.astype(BF16))
            rows.append(refs[2 * e + near][0])
    out_ref[...] = dot(jnp.concatenate(picks, axis=1), jnp.concatenate(rows, axis=0))


def token_sums(lo, hi, pos, r):
    experts, blocks = pos.shape[:2]
    dim = r.shape[2]
    specs = []
    for e in range(experts):
        specs.append(pl.BlockSpec((1, TB, dim), lambda b, l, h, e=e: (e, l[e, b], 0)))
        specs.append(pl.BlockSpec((1, TB, dim), lambda b, l, h, e=e: (e, h[e, b], 0)))
    return pl.pallas_call(
        functools.partial(token_sum_kernel, experts),
        grid_spec=pltpu.PrefetchScalarGridSpec(
            num_scalar_prefetch=2, grid=(blocks,),
            in_specs=[pl.BlockSpec((experts, 1, 1, TB), lambda b, l, h: (0, b, 0, 0))] + specs,
            out_specs=[pl.BlockSpec((TB, dim), lambda b, l, h: (b, 0))]),
        out_shape=[jax.ShapeDtypeStruct((blocks * TB, dim), F32)],
        compiler_params=params(1),
        cost_estimate=pl.CostEstimate(flops=20_000_000_000, bytes_accessed=100_000_000, transcendentals=0),
        name="token_sums",
    )(lo, hi, pos, *([r] * (2 * experts)))[0]


def shared_backward(x, dy, gate_w, up_w, down_w):
    x, dy = x[None], dy[None]
    tokens = x.shape[1]
    tm = tokens // 4
    tiles = jnp.arange(tokens // TM, dtype=I32)[None]
    ones = jnp.ones_like(tiles)
    hidden, grads, back = ffn_tiles(jnp.full((1,), 4, I32), x, dy, gate_w[None], up_w[None], down_w[None], F32, (tm,), 1, 0, (), "shared_ffn")
    grad_gate, grad_up = up_grads(tiles, ones, x, grads, 4, (TM,))
    grad_down = down_grads(tiles, ones, hidden, dy, 2, (TM,))
    return back[0], grad_gate, grad_up, grad_down


def chunk_tables(codes, gates, experts):
    top_k, tokens = codes.shape
    blocks = tokens // TB
    ids = lax.axis_index('ep') * experts + jnp.arange(experts, dtype=I32)
    match = codes[None] == ids[:, None, None].astype(F32)
    hit = jnp.any(match, axis=1).reshape(experts, blocks, TB)
    gate = jnp.sum(jnp.where(match, gates[None], 0.0), axis=1).reshape(experts, blocks, 1, TB)
    tri = (jnp.arange(TB)[:, None] < jnp.arange(TB)[None, :]).astype(BF16)
    rank = jnp.dot(hit.reshape(-1, TB).astype(BF16), tri, preferred_element_type=F32).astype(I32).reshape(experts, blocks, TB)
    count = jnp.sum(hit.astype(I32), axis=2)
    below = jnp.arange(blocks)[:, None] < jnp.arange(blocks)[None, :]
    start = jnp.sum(jnp.where(below[None], count[:, :, None], 0), axis=1)
    total = start[:, -1] + count[:, -1]
    pos = jnp.where(hit, start[:, :, None] + rank, -(1 << 20)).reshape(experts, blocks, 1, TB)
    units = jnp.maximum((total + TB - 1) // TB, 1)
    lo = jnp.minimum(start // TB, units[:, None] - 1)
    hi = jnp.minimum(lo + 1, units[:, None] - 1)
    fine = jnp.sum(hit.reshape(experts, tokens // 128, 128).astype(I32), axis=2)
    spans = tokens // 128
    fine_start = jnp.sum(jnp.where((jnp.arange(spans)[:, None] < jnp.arange(spans)[None, :])[None], fine[:, :, None], 0), axis=1)
    edge = jnp.arange(blocks, dtype=I32)[None, :, None] * TB
    first = jnp.sum((fine_start + fine)[:, None, :] <= edge, axis=2).astype(I32)
    inside = (fine_start[:, None, :] < edge + TB) & (fine_start < total[:, None])[:, None, :]
    last = jnp.sum(inside, axis=2).astype(I32) - 1
    windows = jnp.maximum(((last - first + 1) * 128 + WINDOW - 1) // WINDOW, 1)
    return first * 128, windows, units, lo, hi, pos, gate


def solution(mesh):
    group = mesh.shape['ep']
    token_spec = P(('dp', 'ep'), None)
    expert_spec = P('ep', None, None)
    whole_spec = P(None, None)
    grad_spec = P(('dp', 'ep'), None, None)

    def local_backward(x_tokens, dy_tokens, expert_ids, gate_vals, slot_pos, w_gate, w_up, w_down, shared_gate, shared_up, shared_down):
        tok_count, top_k = expert_ids.shape
        local_experts = w_gate.shape[0]
        part = tok_count // CHUNKS
        codes = jnp.where(slot_pos >= 0, expert_ids, -1).astype(F32).T
        plan = lax.all_gather(jnp.concatenate([codes, gate_vals.T], axis=0), 'ep', axis=0)
        gathered = []
        for c in range(CHUNKS):
            rows = slice(c * part, (c + 1) * part)
            gathered.append((lax.all_gather(x_tokens[rows], 'ep', axis=0, tiled=True), lax.all_gather(dy_tokens[rows], 'ep', axis=0, tiled=True)))
        shared = shared_backward(x_tokens, dy_tokens, shared_gate, shared_up, shared_down)
        shared_dx, grad_shared_gate, grad_shared_up, grad_shared_down = shared
        packed, wide, summed, units, after = (), (), [], [], shared[1:]
        for c in range(CHUNKS):
            mine = plan[:, :, c * part:(c + 1) * part].transpose(1, 0, 2).reshape(2 * top_k, group * part)
            first, windows, count, lo, hi, pos, gate = chunk_tables(mine[:top_k], mine[top_k:], local_experts)
            packed = pack_rows(first, windows, count, *gathered[c], pos.reshape(local_experts, 1, -1), gate.reshape(local_experts, 1, -1), c, packed, after)
            *wide, back = ffn_tiles(count, *packed, w_gate, w_up, w_down, BF16, (TB, TM), CHUNKS, c, wide, "ffn_tiles")
            sums = token_sums(lo, hi, pos, back)
            after = (sums,)
            summed.append(lax.psum_scatter(sums, 'ep', scatter_dimension=0, tiled=True))
            units.append(count)
        capacity = (3 * tok_count * top_k + 2 * local_experts * group - 1) // (2 * local_experts * group)
        steps = min(CHUNKS * group * part // TM, (group * capacity + CHUNKS * (TM - 1)) // TM)
        tiles, left = gradient_tiles(jnp.stack(units), group * part // TM, steps)
        x_rows, z_rows = packed
        hidden, grads = wide
        grad_w_gate, grad_w_up = up_grads(tiles, left, x_rows, grads, 2, (TB, TM))
        grad_w_down = down_grads(tiles, left, hidden, z_rows, 1, (TB, TM))
        grad_x = (jnp.concatenate(summed, axis=0) + shared_dx).astype(BF16)
        return grad_x, grad_w_gate, grad_w_up, grad_w_down, grad_shared_gate, grad_shared_up, grad_shared_down

    return jax.shard_map(local_backward, mesh=mesh, in_specs=(token_spec, token_spec, token_spec, token_spec, token_spec, expert_spec, expert_spec, expert_spec, whole_spec, whole_spec, whole_spec), out_specs=(token_spec, grad_spec, grad_spec, grad_spec, grad_spec, grad_spec, grad_spec), check_vma=False)
```

```python
import functools

import jax
import jax.numpy as jnp
from jax import lax
from jax.experimental import pallas as pl
from jax.experimental.pallas import tpu as pltpu
from jax.sharding import PartitionSpec as P

BF16, F32, I32 = jnp.bfloat16, jnp.float32, jnp.int32
TB = 256
TM = 512
WINDOW = 768
CHUNKS = 3
VMEM = 64 * 1024 * 1024 - 128 * 1024


def dot(a, b):
    return lax.dot_general(a, b, (((1,), (0,)), ((), ())), preferred_element_type=F32)


def dot_t(a, b):
    return lax.dot_general(a, b, (((1,), (1,)), ((), ())), preferred_element_type=F32)


def params(ndim):
    return pltpu.CompilerParams(dimension_semantics=("arbitrary",) * ndim, vmem_limit_bytes=VMEM)


def swiglu_parts(act_gate, act_up, grad_hidden):
    gate_f32 = act_gate.astype(F32)
    up_f32 = act_up.astype(F32)
    sigma = jax.nn.sigmoid(gate_f32)
    silu_gate = gate_f32 * sigma
    hidden = (silu_gate * up_f32).astype(BF16)
    grad_gate = (grad_hidden * up_f32 * sigma * (1.0 + gate_f32 * (1.0 - sigma))).astype(BF16)
    grad_up = (grad_hidden * silu_gate).astype(BF16)
    return hidden, grad_gate, grad_up


def pack_kernel(first_ref, window_ref, n_ref, x_ref, dy_ref, pos_ref, gate_ref, *refs):
    xo_ref, zo_ref = refs[-2:]
    e, m = pl.program_id(0), pl.program_id(1)
    tokens = x_ref.shape[0]

    def window(w):
        wanted = first_ref[e, m] + w * WINDOW
        begin = pl.multiple_of(jnp.minimum(wanted, tokens - WINDOW), 128)
        at = pl.ds(begin, WINDOW)
        token = begin + lax.broadcasted_iota(I32, (1, WINDOW), 1)
        local = jnp.where(token >= wanted, pos_ref[0, :, at] - m * TB, -1)
        hit = lax.broadcasted_iota(I32, (TB, WINDOW), 0) == local
        row_gate = jnp.sum(jnp.where(hit, gate_ref[0, :, at], 0.0), axis=1, keepdims=True)
        pick = hit.astype(F32).astype(BF16)
        return dot(pick, x_ref[at, :]).astype(BF16), (dot(pick, dy_ref[at, :]) * row_gate).astype(BF16)

    @pl.when(m < n_ref[e])
    def _():
        xo_ref[0], zo_ref[0] = window(0)

    def more(w, carry):
        x_rows, z_rows = window(w)
        xo_ref[0] += x_rows
        zo_ref[0] += z_rows
        return carry

    lax.fori_loop(1, jnp.where(m < n_ref[e], window_ref[e, m], 1), more, 0)


def pack_rows(first, windows, units, x, dy, pos, gate, chunk, held, after):
    experts = pos.shape[0]
    rows, dim = x.shape
    tok = pl.BlockSpec((rows, dim), lambda e, m, f, w, n: (0, 0), pipeline_mode=pl.Buffered(1))
    row = pl.BlockSpec((1, 1, rows), lambda e, m, f, w, n: (e, 0, 0))
    out = pl.BlockSpec((1, TB, dim), lambda e, m, f, w, n: (e, chunk * (rows // TB) + jnp.minimum(m, n[e] - 1), 0))
    return pl.pallas_call(
        pack_kernel,
        grid_spec=pltpu.PrefetchScalarGridSpec(
            num_scalar_prefetch=3, grid=(experts, rows // TB),
            in_specs=[tok, tok, row, row] + [pl.BlockSpec(memory_space=pl.ANY)] * (len(held) + len(after)),
            out_specs=[out, out]),
        out_shape=[jax.ShapeDtypeStruct((experts, CHUNKS * rows, dim), BF16)] * 2,
        input_output_aliases={7 + i: i for i in range(len(held))},
        compiler_params=params(2),
        cost_estimate=pl.CostEstimate(flops=30_000_000_000, bytes_accessed=200_000_000, transcendentals=0),
        name="pack_rows",
    )(first, windows, units, x, dy, pos, gate, *held, *after)


def ffn_kernel(sizes, n_ref, x_ref, z_ref, w1_ref, w3_ref, w2_ref, *refs):
    h_ref, d_ref, r_ref = refs[-3:]
    ff = w1_ref.shape[2]
    dim = w1_ref.shape[1]
    left = n_ref[pl.program_id(0)] - len(sizes) * pl.program_id(1)

    def tile(rows):
        def columns(lo, size, act_gate, act_up):
            grad_hidden = dot_t(z_ref[0, :rows], w2_ref[0, lo:lo + size, :])
            hidden, grad_gate, grad_up = swiglu_parts(act_gate.astype(BF16), act_up.astype(BF16), grad_hidden)
            h_ref[0, :rows, lo:lo + size] = hidden
            d_ref[0, :rows, lo:lo + size] = grad_gate
            d_ref[0, :rows, ff + lo:ff + lo + size] = grad_up

        full = ff // 256 * 256
        for lo in range(0, full, 256):
            columns(lo, 256, dot(x_ref[0, :rows], w1_ref[0, :, lo:lo + 256]), dot(x_ref[0, :rows], w3_ref[0, :, lo:lo + 256]))
        if full < ff:
            both = dot(x_ref[0, :rows], jnp.concatenate([w1_ref[0, :, full:], w3_ref[0, :, full:]], axis=1))
            columns(full, ff - full, both[:, :ff - full], both[:, ff - full:])
        for lo in range(0, dim, 256):
            w = jnp.concatenate([w1_ref[0, lo:lo + 256, :], w3_ref[0, lo:lo + 256, :]], axis=1)
            r_ref[0, :rows, lo:lo + 256] = dot_t(d_ref[0, :rows], w).astype(r_ref.dtype)

    for i, rows in enumerate(sizes):
        pl.when((left == i + 1) if i + 1 < len(sizes) else (left > i))(functools.partial(tile, rows))


def ffn_tiles(units, x, z, w1, w3, w2, out_dtype, sizes, chunks, chunk, held, name):
    experts, dim, ff = w1.shape
    rows = x.shape[1] // chunks
    tm, per = sizes[-1], len(sizes)
    inner = lambda e, m, n: jnp.minimum(m, (n[e] + per - 1) // per - 1)
    tile = lambda e, m, n: (e, chunk * (rows // tm) + inner(e, m, n), 0)
    whole = lambda e, m, n: (e, 0, 0)
    depth = pl.Buffered(min(experts, 2))
    return pl.pallas_call(
        functools.partial(ffn_kernel, sizes),
        grid_spec=pltpu.PrefetchScalarGridSpec(
            num_scalar_prefetch=1, grid=(experts, rows // tm),
            in_specs=[pl.BlockSpec((1, tm, dim), tile), pl.BlockSpec((1, tm, dim), tile),
                      pl.BlockSpec((1, dim, ff), whole, pipeline_mode=depth),
                      pl.BlockSpec((1, dim, ff), whole, pipeline_mode=depth),
                      pl.BlockSpec((1, ff, dim), whole, pipeline_mode=depth)] + [pl.BlockSpec(memory_space=pl.ANY)] * len(held),
            out_specs=[pl.BlockSpec((1, tm, ff), tile), pl.BlockSpec((1, tm, 2 * ff), tile),
                       pl.BlockSpec((1, tm, dim), lambda e, m, n: (e, inner(e, m, n), 0))]),
        out_shape=[jax.ShapeDtypeStruct((experts, chunks * rows, ff), BF16),
                   jax.ShapeDtypeStruct((experts, chunks * rows, 2 * ff), BF16),
                   jax.ShapeDtypeStruct((experts, rows, dim), out_dtype)],
        input_output_aliases={6 + i: i for i in range(len(held))},
        compiler_params=params(2),
        cost_estimate=pl.CostEstimate(flops=5 * experts * rows * dim * ff, bytes_accessed=150_000_000, transcendentals=0),
        name=name,
    )(units, x, z, w1, w3, w2, *held)


def for_tile(sizes, left_ref, body):
    left = left_ref[pl.program_id(0), pl.program_id(2)]
    for i, rows in enumerate(sizes):
        pl.when((left == i + 1) if i + 1 < len(sizes) else (left > i))(functools.partial(body, rows))


def up_grad_kernel(sizes, tile_ref, left_ref, x_ref, d_ref, g1_ref, g3_ref):
    ff = g1_ref.shape[2]

    @pl.when(pl.program_id(2) == 0)
    def _():
        g1_ref[...] = jnp.zeros_like(g1_ref)
        g3_ref[...] = jnp.zeros_like(g3_ref)

    def body(rows):
        x_t = x_ref[0, :rows].T
        for lo in range(0, 2 * ff, 256):
            part = dot(x_t, d_ref[0, :rows, lo:lo + 256])
            if lo + 256 <= ff:
                g1_ref[0, :, lo:lo + 256] += part
            elif lo >= ff:
                g3_ref[0, :, lo - ff:lo - ff + 256] += part
            else:
                g1_ref[0, :, lo:] += part[:, :ff - lo]
                g3_ref[0, :, :lo + 256 - ff] += part[:, ff - lo:]

    for_tile(sizes, left_ref, body)


def up_grads(tiles, left, x, d, split, sizes):
    experts, _, dim = x.shape
    ff = d.shape[2] // 2
    out = lambda e, s, j, t, n: (e, s, 0)
    return pl.pallas_call(
        functools.partial(up_grad_kernel, sizes),
        grid_spec=pltpu.PrefetchScalarGridSpec(
            num_scalar_prefetch=2, grid=(experts, split, tiles.shape[1]),
            in_specs=[pl.BlockSpec((1, TM, dim // split), lambda e, s, j, t, n: (e, t[e, j], s)),
                      pl.BlockSpec((1, TM, 2 * ff), lambda e, s, j, t, n: (e, t[e, j], 0))],
            out_specs=[pl.BlockSpec((1, dim // split, ff), out)] * 2),
        out_shape=[jax.ShapeDtypeStruct((experts, dim, ff), F32)] * 2,
        compiler_params=params(3),
        cost_estimate=pl.CostEstimate(flops=120_000_000_000, bytes_accessed=250_000_000, transcendentals=0),
        name="up_grads",
    )(tiles, left, x, d)


def down_grad_kernel(sizes, tile_ref, left_ref, h_ref, z_ref, g_ref):
    @pl.when(pl.program_id(2) == 0)
    def _():
        g_ref[...] = jnp.zeros_like(g_ref)

    def body(rows):
        h_t = h_ref[0, :rows].T
        for lo in range(0, g_ref.shape[2], 256):
            g_ref[0, :, lo:lo + 256] += dot(h_t, z_ref[0, :rows, lo:lo + 256])

    for_tile(sizes, left_ref, body)


def down_grads(tiles, left, h, z, split, sizes):
    experts, _, ff = h.shape
    dim = z.shape[2]
    return pl.pallas_call(
        functools.partial(down_grad_kernel, sizes),
        grid_spec=pltpu.PrefetchScalarGridSpec(
            num_scalar_prefetch=2, grid=(experts, split, tiles.shape[1]),
            in_specs=[pl.BlockSpec((1, TM, ff), lambda e, s, j, t, n: (e, t[e, j], 0)),
                      pl.BlockSpec((1, TM, dim // split), lambda e, s, j, t, n: (e, t[e, j], s))],
            out_specs=[pl.BlockSpec((1, ff, dim // split), lambda e, s, j, t, n: (e, 0, s))]),
        out_shape=[jax.ShapeDtypeStruct((experts, ff, dim), F32)],
        compiler_params=params(3),
        cost_estimate=pl.CostEstimate(flops=60_000_000_000, bytes_accessed=150_000_000, transcendentals=0),
        name="down_grads",
    )(tiles, left, h, z)[0]


def gradient_tiles(units, chunk_tiles, steps):
    per = TM // TB
    tiles = (units + per - 1) // per
    ends = jnp.cumsum(tiles, axis=0)
    j = jnp.arange(steps, dtype=I32)
    j_in = jnp.minimum(j[None, :], ends[-1][:, None] - 1)
    chunk = jnp.sum((j_in[None] >= ends[:, :, None]).astype(I32), axis=0)
    begin = jnp.sum(jnp.where(jnp.arange(len(units))[:, None, None] < chunk[None], tiles[:, :, None], 0), axis=0)
    count = jnp.sum(jnp.where(jnp.arange(len(units))[:, None, None] == chunk[None], units[:, :, None], 0), axis=0)
    inner = j_in - begin
    left = jnp.where(j[None, :] < ends[-1][:, None], count - per * inner, 0)
    return (chunk * chunk_tiles + inner).astype(I32), left.astype(I32)


def token_sum_kernel(experts, lo_ref, hi_ref, pos_ref, *refs):
    b = pl.program_id(0)
    out_ref = refs[-1]
    picks, rows = [], []
    for e in range(experts):
        for near in range(2):
            tile = hi_ref[e, b] if near else lo_ref[e, b]
            local = pos_ref[e, 0] - tile * TB
            if near:
                local = jnp.where(tile == lo_ref[e, b], -1, local)
            picks.append((lax.broadcasted_iota(I32, (TB, TB), 0) == local).astype(F32).astype(BF16))
            rows.append(refs[2 * e + near][0])
    out_ref[...] = lax.dot_general(jnp.concatenate(picks, axis=0), jnp.concatenate(rows, axis=0), (((0,), (0,)), ((), ())), preferred_element_type=F32)


def token_sums(lo, hi, pos, r):
    experts, blocks = pos.shape[:2]
    dim = r.shape[2]
    specs = []
    for e in range(experts):
        specs.append(pl.BlockSpec((1, TB, dim), lambda b, l, h, e=e: (e, l[e, b], 0)))
        specs.append(pl.BlockSpec((1, TB, dim), lambda b, l, h, e=e: (e, h[e, b], 0)))
    return pl.pallas_call(
        functools.partial(token_sum_kernel, experts),
        grid_spec=pltpu.PrefetchScalarGridSpec(
            num_scalar_prefetch=2, grid=(blocks,),
            in_specs=[pl.BlockSpec((experts, 1, 1, TB), lambda b, l, h: (0, b, 0, 0))] + specs,
            out_specs=[pl.BlockSpec((TB, dim), lambda b, l, h: (b, 0))]),
        out_shape=[jax.ShapeDtypeStruct((blocks * TB, dim), F32)],
        compiler_params=params(1),
        cost_estimate=pl.CostEstimate(flops=20_000_000_000, bytes_accessed=100_000_000, transcendentals=0),
        name="token_sums",
    )(lo, hi, pos, *([r] * (2 * experts)))[0]


def shared_backward(x, dy, gate_w, up_w, down_w):
    x, dy = x[None], dy[None]
    tokens = x.shape[1]
    tm = tokens // 4
    tiles = jnp.arange(tokens // TM, dtype=I32)[None]
    ones = jnp.ones_like(tiles)
    hidden, grads, back = ffn_tiles(jnp.full((1,), 4, I32), x, dy, gate_w[None], up_w[None], down_w[None], F32, (tm,), 1, 0, (), "shared_ffn")
    grad_gate, grad_up = up_grads(tiles, ones, x, grads, 4, (TM,))
    grad_down = down_grads(tiles, ones, hidden, dy, 2, (TM,))
    return back[0], grad_gate, grad_up, grad_down


def chunk_tables(codes, gates, experts):
    top_k, tokens = codes.shape
    blocks = tokens // TB
    ids = lax.axis_index('ep') * experts + jnp.arange(experts, dtype=I32)
    match = codes[None] == ids[:, None, None].astype(F32)
    hit = jnp.any(match, axis=1).reshape(experts, blocks, TB)
    gate = jnp.sum(jnp.where(match, gates[None], 0.0), axis=1).reshape(experts, blocks, 1, TB)
    tri = (jnp.arange(TB)[:, None] < jnp.arange(TB)[None, :]).astype(BF16)
    rank = jnp.dot(hit.reshape(-1, TB).astype(BF16), tri, preferred_element_type=F32).astype(I32).reshape(experts, blocks, TB)
    count = jnp.sum(hit.astype(I32), axis=2)
    below = jnp.arange(blocks)[:, None] < jnp.arange(blocks)[None, :]
    start = jnp.sum(jnp.where(below[None], count[:, :, None], 0), axis=1)
    total = start[:, -1] + count[:, -1]
    pos = jnp.where(hit, start[:, :, None] + rank, -(1 << 20)).reshape(experts, blocks, 1, TB)
    units = jnp.maximum((total + TB - 1) // TB, 1)
    lo = jnp.minimum(start // TB, units[:, None] - 1)
    hi = jnp.minimum(lo + 1, units[:, None] - 1)
    fine = jnp.sum(hit.reshape(experts, tokens // 128, 128).astype(I32), axis=2)
    spans = tokens // 128
    fine_start = jnp.sum(jnp.where((jnp.arange(spans)[:, None] < jnp.arange(spans)[None, :])[None], fine[:, :, None], 0), axis=1)
    edge = jnp.arange(blocks, dtype=I32)[None, :, None] * TB
    first = jnp.sum((fine_start + fine)[:, None, :] <= edge, axis=2).astype(I32)
    inside = (fine_start[:, None, :] < edge + TB) & (fine_start < total[:, None])[:, None, :]
    last = jnp.sum(inside, axis=2).astype(I32) - 1
    windows = jnp.maximum(((last - first + 1) * 128 + WINDOW - 1) // WINDOW, 1)
    return first * 128, windows, units, lo, hi, pos, gate


def solution(mesh):
    group = mesh.shape['ep']
    token_spec = P(('dp', 'ep'), None)
    expert_spec = P('ep', None, None)
    whole_spec = P(None, None)
    grad_spec = P(('dp', 'ep'), None, None)

    def local_backward(x_tokens, dy_tokens, expert_ids, gate_vals, slot_pos, w_gate, w_up, w_down, shared_gate, shared_up, shared_down):
        tok_count, top_k = expert_ids.shape
        local_experts = w_gate.shape[0]
        part = tok_count // CHUNKS
        codes = jnp.where(slot_pos >= 0, expert_ids, -1).astype(F32).T
        plan = lax.all_gather(jnp.concatenate([codes, gate_vals.T, jnp.zeros((24 - 2 * top_k, tok_count), F32)], axis=0), 'ep', axis=0)
        gathered = []
        for c in range(CHUNKS):
            rows = slice(c * part, (c + 1) * part)
            gathered.append((lax.all_gather(x_tokens[rows], 'ep', axis=0, tiled=True), lax.all_gather(dy_tokens[rows], 'ep', axis=0, tiled=True)))
        shared = shared_backward(x_tokens, dy_tokens, shared_gate, shared_up, shared_down)
        shared_dx, grad_shared_gate, grad_shared_up, grad_shared_down = shared
        packed, wide, summed, units, after = (), (), [], [], shared[1:]
        for c in range(CHUNKS):
            mine = plan[:, :2 * top_k, c * part:(c + 1) * part].transpose(1, 0, 2).reshape(2 * top_k, group * part)
            first, windows, count, lo, hi, pos, gate = chunk_tables(mine[:top_k], mine[top_k:], local_experts)
            packed = pack_rows(first, windows, count, *gathered[c], pos.reshape(local_experts, 1, -1), gate.reshape(local_experts, 1, -1), c, packed, after)
            *wide, back = ffn_tiles(count, *packed, w_gate, w_up, w_down, BF16, (TB, TM), CHUNKS, c, wide, "ffn_tiles")
            sums = token_sums(lo, hi, pos, back)
            after = (sums,)
            summed.append(lax.psum_scatter(sums, 'ep', scatter_dimension=0, tiled=True))
            units.append(count)
        capacity = (3 * tok_count * top_k + 2 * local_experts * group - 1) // (2 * local_experts * group)
        steps = min(CHUNKS * group * part // TM, (group * capacity + CHUNKS * (TM - 1)) // TM)
        tiles, left = gradient_tiles(jnp.stack(units), group * part // TM, steps)
        x_rows, z_rows = packed
        hidden, grads = wide
        grad_w_gate, grad_w_up = up_grads(tiles, left, x_rows, grads, 2, (TB, TM))
        grad_w_down = down_grads(tiles, left, hidden, z_rows, 1, (TB, TM))
        grad_x = (jnp.concatenate(summed, axis=0) + shared_dx).astype(BF16)
        return grad_x, grad_w_gate, grad_w_up, grad_w_down, grad_shared_gate, grad_shared_up, grad_shared_down

    return jax.shard_map(local_backward, mesh=mesh, in_specs=(token_spec, token_spec, token_spec, token_spec, token_spec, expert_spec, expert_spec, expert_spec, whole_spec, whole_spec, whole_spec), out_specs=(token_spec, grad_spec, grad_spec, grad_spec, grad_spec, grad_spec, grad_spec), check_vma=False)
```
